32 devices in a mesh: job: 4 (over y, x), zero: 2 (over core), cols: 4 (over z).
Axes of the slice: x: 2, y: 2, z: 4, core: 2. Of those that a mesh axis runs over, the one named last changes fastest.
Arguments:
- weight_gate: bfloat16 [8192, 8192], P(('job', 'zero'), 'cols'), parts along dimension 0, may hold values from -0.1875 to 0.1875
- low_gate: bfloat16 [8192, 32], P(('job', 'zero')), parts along dimension 0, may hold values from -0.125 to 0.125
- high_gate: bfloat16 [128, 8192], P('job', 'cols'), parts along dimension 0, may hold values from -1 to 1
- weight_up: bfloat16 [8192, 8192], P(('job', 'zero'), 'cols'), parts along dimension 0, may hold values from -0.1875 to 0.1875
- low_up: bfloat16 [8192, 32], P(('job', 'zero')), parts along dimension 0, may hold values from -0.125 to 0.125
- high_up: bfloat16 [128, 8192], P('job', 'cols'), parts along dimension 0, may hold values from -1 to 1
- norm_train: float32 [8192], P(('job', 'zero', 'cols')), parts along dimension 0, may hold values from 0.25 to 1.75
- norm_step: float32 [8192], P(('job', 'zero', 'cols')), parts along dimension 0, may hold values from -0.3 to 0.3
Outputs:
- serving_gate: bfloat16 [8192, 8192], P('job', 'cols'), parts along dimension 0
- serving_up: bfloat16 [8192, 8192], P('job', 'cols'), parts along dimension 0
- column_gate: float32 [32768], P(('job', 'cols')), parts along dimension 0
- column_up: float32 [32768], P(('job', 'cols')), parts along dimension 0
- serve_norm: bfloat16 [8192], P('job'), parts along dimension 0
The draws below stay inside these ranges and needn't reach their ends.
There are 4 independent parts, one for each index of `job`. The reference program is written for one: setup_inputs(seed, part) draws one part's arguments, and reference() takes and returns one part's arrays. A program takes and returns all parts, laid end to end along the dimension named above; each array names one. Nothing has to cross between parts.
All inputs are finite; a program needn't handle non-finite values. Where the reference program divides by a largest or mean magnitude, that divisor is 1e-20 or more.
Results may differ from the reference program's by a relative error of at most 0.001.
Values may be sent and summed in bfloat16 or wider, within the bound.
No kernel may reach another device: no remote copies, remote signals or barrier semaphores. Data moves between devices by JAX's collectives and lax.ppermute only.
A program may use at most 128 MiB of HBM per device.

```python
import jax
import jax.numpy as jnp

D_MODEL = 2048
D_INNER = 8192
RANK = 32


def raised(array, own_key, source, target, blocks, factor):
    def block_of(position):
        return (jnp.arange(array.shape[position]) // (array.shape[position] // blocks)).reshape((-1,) + (1,) * (array.ndim - 1 - position))

    one_side = jax.random.permutation(own_key, blocks)[block_of(target)]
    second = (block_of(target) + blocks // 2) % blocks
    return jnp.where((block_of(source) == one_side) | (block_of(source) == second), factor * array, array)


def level_of(key, dims, pieces, smallest, largest):
    def one(position, shards_of):
        draws = jax.random.uniform(jax.random.fold_in(jax.random.fold_in(key, 6), position), (shards_of,), jnp.float32, smallest / len(pieces), largest / len(pieces))
        return jnp.repeat(jnp.exp(draws), dims[position] // shards_of).reshape((-1,) + (1,) * (len(dims) - position - 1))

    level = one(*pieces[0])
    for cut in pieces[1:]:
        level = level * one(*cut)
    return level


def normal_values(rng, dims, scale, bound, pieces=(), dtype=jnp.bfloat16):
    entries = scale * jax.random.normal(rng, dims, jnp.float32)
    if pieces:
        entries = entries * level_of(rng, dims, pieces, -0.22, 0.18)
    return jnp.clip(entries, -bound, bound).astype(dtype)


def gaussian_with(own_key, dims, deviation, most, split, heavy, held_as=jnp.bfloat16):
    array = deviation * jax.random.normal(own_key, dims, jnp.float32)
    if split:
        array = array * level_of(own_key, dims, split, -0.22, 0.18)
    return jnp.clip(raised(array, jax.random.fold_in(own_key, 3), *heavy), -most, most).astype(held_as)


def setup_inputs(seed: int = 0, part: int = 0) -> dict:
    keys = jax.random.split(jax.random.key(seed), 9)
    part_keys = jax.random.split(jax.random.fold_in(keys[8], part), 9)
    weight_gate = gaussian_with(part_keys[0], (D_MODEL, D_INNER), D_MODEL ** -0.5, 0.1875, ((0, 2), (1, 4)), (0, 1, 4, 2.0))
    low_gate = normal_values(part_keys[1], (D_MODEL, RANK), D_MODEL ** -0.5, 0.125, ((0, 2),))
    high_gate = normal_values(part_keys[2], (RANK, D_INNER), RANK ** -0.5, 1.0, ((1, 4),))
    weight_up = gaussian_with(part_keys[3], (D_MODEL, D_INNER), D_MODEL ** -0.5, 0.1875, ((0, 2), (1, 4)), (0, 1, 4, 2.0))
    low_up = normal_values(part_keys[4], (D_MODEL, RANK), D_MODEL ** -0.5, 0.125, ((0, 2),))
    high_up = normal_values(part_keys[5], (RANK, D_INNER), RANK ** -0.5, 1.0, ((1, 4),))
    norm_train = jnp.clip(1.0 + 0.15 * jax.random.normal(part_keys[6], (D_MODEL,), jnp.float32), 0.25, 1.75)
    norm_step = jnp.clip(jax.random.uniform(part_keys[7], (D_MODEL,), jnp.float32, -0.3, 0.3) * level_of(part_keys[7], (D_MODEL,), ((0, 8),), -0.4, 0.0), -0.3, 0.3)
    return {"weight_gate": weight_gate, "low_gate": low_gate, "high_gate": high_gate, "weight_up": weight_up, "low_up": low_up, "high_up": high_up, "norm_train": norm_train, "norm_step": norm_step}


mix_rate = 2.0


def reference(weight_gate, low_gate, high_gate, weight_up, low_up, high_up, norm_train, norm_step):
    whole_gate = weight_gate.astype(jnp.float32) + mix_rate * jnp.dot(low_gate, high_gate, preferred_element_type=jnp.float32)
    whole_up = weight_up.astype(jnp.float32) + mix_rate * jnp.dot(low_up, high_up, preferred_element_type=jnp.float32)
    column_gate = jnp.max(jnp.abs(whole_gate), axis=0)
    serving_gate = (whole_gate / column_gate).astype(jnp.bfloat16)
    column_up = jnp.max(jnp.abs(whole_up), axis=0)
    serving_up = (whole_up / column_up).astype(jnp.bfloat16)
    serve_norm = (norm_train + norm_step).astype(jnp.bfloat16)
    return serving_gate, serving_up, column_gate, column_up, serve_norm
```

```python
import functools

import jax
import jax.numpy as jnp
from jax import lax
from jax.experimental import pallas as pl
from jax.experimental.pallas import tpu as pltpu
from jax.sharding import PartitionSpec as P

mix_rate = 2.0


def merge_kernel(shards, tile, *refs):
    weights, lows = refs[:shards], refs[shards : 2 * shards]
    high_ref, out_ref, column_ref, whole = refs[2 * shards :]
    me = lax.axis_index("zero")
    rows = weights[0].shape[0]
    high = high_ref[...] * jnp.asarray(mix_rate, high_ref.dtype)
    peak = jnp.zeros((8, high.shape[1]), jnp.float32)
    for shift in range(shards):
        low = lows[shift][...]
        for start in range(0, rows, tile):
            piece = lax.dot_general(
                low[:, start : start + tile],
                high,
                (((0,), (0,)), ((), ())),
                preferred_element_type=jnp.float32,
            ) + weights[shift][pl.ds(start, tile), :].astype(jnp.float32)
            whole[pl.ds(shift * rows + start, tile), :] = piece
            peak = jnp.maximum(peak, jnp.max(jnp.abs(piece).reshape(tile // 8, 8, -1), axis=0))
    column = jnp.max(peak, axis=0, keepdims=True)
    column_ref[...] = column
    inverse = 1.0 / column
    for shift in range(shards):
        owner = lax.rem(me - shift + shards, shards)
        base = pl.multiple_of(owner * rows, rows)
        for start in range(0, rows, tile):
            out_ref[pl.ds(base + start, tile), :] = (
                whole[pl.ds(shift * rows + start, tile), :] * inverse
            ).astype(out_ref.dtype)


def merge(weights, lows, high):
    shards = len(weights)
    rows, columns = weights[0].shape
    rank = high.shape[0]
    block = min(256, columns)
    tile = min(128, rows)
    total = shards * rows
    return pl.pallas_call(
        functools.partial(merge_kernel, shards, tile),
        grid=(columns // block,),
        out_shape=(
            jax.ShapeDtypeStruct((total, columns), jnp.bfloat16),
            jax.ShapeDtypeStruct((1, columns), jnp.float32),
        ),
        in_specs=[pl.BlockSpec((rows, block), lambda j: (0, j))] * shards
        + [pl.BlockSpec((rank, rows), lambda j: (0, 0))] * shards
        + [pl.BlockSpec((rank, block), lambda j: (0, j))],
        out_specs=(
            pl.BlockSpec((total, block), lambda j: (0, j)),
            pl.BlockSpec((1, block), lambda j: (0, j)),
        ),
        scratch_shapes=[pltpu.VMEM((total, block), jnp.float32)],
        compiler_params=pltpu.CompilerParams(
            dimension_semantics=("arbitrary",), vmem_limit_bytes=20 * 1024 * 1024
        ),
        cost_estimate=pl.CostEstimate(
            flops=2 * total * columns * 256,
            bytes_accessed=4 * total * columns,
            transcendentals=0,
        ),
        name="merge",
    )(*weights, *lows, high)


def norm_kernel(shards, *refs):
    pieces, out_ref, held = refs[:shards], refs[shards], refs[shards + 1]
    me = lax.axis_index(("zero", "cols"))
    rows = pieces[0].shape[0]
    for shift in range(shards):
        owner = lax.rem(me - shift + shards, shards)
        held[pl.ds(owner * rows, rows), :] = pieces[shift][...]
    out_ref[...] = held[...].astype(out_ref.dtype)


def passed_round(array, axes, shards):
    return [array] + [
        lax.ppermute(array, axes, [(i, (i + shift) % shards) for i in range(shards)])
        for shift in range(1, shards)
    ]


def gathered_norm(norm, axes, shards):
    if shards > 8 or norm.shape[0] % 128:
        return lax.all_gather(norm.astype(jnp.bfloat16), axes, axis=0, tiled=True)
    rows = norm.shape[0] // 128
    pieces = passed_round(norm, axes, shards)
    out = pl.pallas_call(
        functools.partial(norm_kernel, shards),
        out_shape=jax.ShapeDtypeStruct((shards * rows, 128), jnp.bfloat16),
        scratch_shapes=[pltpu.VMEM((shards * rows, 128), jnp.float32)],
        compiler_params=pltpu.CompilerParams(vmem_limit_bytes=2 * 1024 * 1024),
        name="norm",
    )(*(piece.reshape(rows, 128) for piece in pieces))
    return out.reshape(-1)


def per_device(
    zero, cols,
    weight_gate, low_gate, high_gate, weight_up, low_up, high_up, norm_train, norm_step,
):
    lows_gate = passed_round(low_gate.T, "zero", zero)
    lows_up = passed_round(low_up.T, "zero", zero)
    weights_gate = passed_round(weight_gate, "zero", zero)
    weights_up = passed_round(weight_up, "zero", zero)
    serve_norm = gathered_norm(norm_train + norm_step, ("zero", "cols"), zero * cols)
    serving_gate, column_gate = merge(weights_gate, lows_gate, high_gate)
    serving_up, column_up = merge(weights_up, lows_up, high_up)
    return (
        serving_gate,
        serving_up,
        column_gate.reshape(-1),
        column_up.reshape(-1),
        serve_norm,
    )


def solution(mesh):
    in_specs = (
        P(("job", "zero"), "cols"),
        P(("job", "zero"), None),
        P("job", "cols"),
        P(("job", "zero"), "cols"),
        P(("job", "zero"), None),
        P("job", "cols"),
        P(("job", "zero", "cols")),
        P(("job", "zero", "cols")),
    )
    out_specs = (
        P("job", "cols"),
        P("job", "cols"),
        P(("job", "cols")),
        P(("job", "cols")),
        P("job"),
    )
    body = functools.partial(per_device, mesh.shape["zero"], mesh.shape["cols"])
    return jax.shard_map(
        body, mesh=mesh, in_specs=in_specs, out_specs=out_specs, check_vma=False
    )
```

```python
import functools

import jax
import jax.numpy as jnp
from jax import lax
from jax.experimental import pallas as pl
from jax.experimental.pallas import tpu as pltpu
from jax.sharding import PartitionSpec as P

mix_rate = 2.0


def merge_kernel(shards, tile, block, fetch, again, *refs):
    own_ref, received, lows = refs[0], refs[1:shards], refs[shards : 2 * shards]
    high_ref, out_ref, column_ref, turned, whole = refs[2 * shards : 2 * shards + 5]
    me = lax.axis_index("zero")
    rows, columns = own_ref.shape
    step = pl.program_id(0)
    here = pl.ds(pl.multiple_of(step * block, block), block)
    weights = (own_ref,) + tuple(received)
    if fetch:
        held, arrived = refs[2 * shards + 5 :]

        def copy(at):
            part = pl.ds(pl.multiple_of(at * block, block), block)
            return pltpu.make_async_copy(own_ref.at[:, part], held.at[:, part], arrived.at[at])

        @pl.when(step == 0)
        def _():
            for at in range(columns // block):
                copy(at).start()

        weights = (held,) + tuple(received)

    @pl.when(step == 0)
    def _():
        for shift in range(shards):
            turned[shift] = lows[shift][...].T

    high = high_ref[...] * jnp.asarray(mix_rate, high_ref.dtype)
    peak = jnp.zeros((8, block), jnp.float32)

    def piece(shift, start):
        return jnp.dot(
            turned[shift, pl.ds(start, tile), :], high, preferred_element_type=jnp.float32
        ) + weights[shift][pl.ds(start, tile), here].astype(jnp.float32)

    for shift in reversed(range(shards)):
        if fetch and shift == 0:
            copy(step).wait()
        for start in range(0, rows, tile):
            merged = piece(shift, start)
            if not again:
                whole[pl.ds(shift * rows + start, tile), :] = merged
            peak = jnp.maximum(peak, jnp.max(jnp.abs(merged).reshape(tile // 8, 8, -1), axis=0))
    column = jnp.max(peak, axis=0, keepdims=True)
    column_ref[...] = column
    inverse = 1.0 / column
    for shift in range(shards):
        owner = lax.rem(me - shift + shards, shards)
        base = pl.multiple_of(owner * rows, rows)
        for start in range(0, rows, tile):
            if again:
                merged = piece(shift, start)
            else:
                merged = whole[pl.ds(shift * rows + start, tile), :]
            out_ref[pl.ds(base + start, tile), :] = (merged * inverse).astype(out_ref.dtype)


def add_kernel(train_ref, step_ref, out_ref):
    out_ref[...] = train_ref[...] + step_ref[...]


def added(norm_train, norm_step, span):
    shape = (norm_train.shape[0] // 128, 128)
    return pl.pallas_call(
        add_kernel,
        out_shape=jax.ShapeDtypeStruct(shape, jnp.float32),
        compiler_params=pltpu.CompilerParams(vmem_limit_bytes=2 * 1024 * 1024),
        cost_estimate=pl.CostEstimate(flops=span * 65536, bytes_accessed=32 * span, transcendentals=0),
        name="added",
    )(norm_train.reshape(shape), norm_step.reshape(shape)).reshape(-1)


def merge(weights, lows, high, fetch, again=False, block=512, tile=128):
    shards = len(weights)
    rows, columns = weights[0].shape
    rank = high.shape[0]
    block = min(block, columns)
    tile = min(tile, rows)
    total = shards * rows
    scratch = [
        pltpu.VMEM((shards, rows, rank), jnp.bfloat16),
        pltpu.VMEM((8 if again else total, block), jnp.float32),
    ]
    if fetch:
        scratch += [
            pltpu.VMEM((rows, columns), weights[0].dtype),
            pltpu.SemaphoreType.DMA((columns // block,)),
        ]
    entire = pl.BlockSpec((rows, columns), lambda j: (0, 0))
    return pl.pallas_call(
        functools.partial(merge_kernel, shards, tile, block, fetch, again),
        grid=(columns // block,),
        out_shape=(
            jax.ShapeDtypeStruct((total, columns), jnp.bfloat16),
            jax.ShapeDtypeStruct((1, columns), jnp.float32),
        ),
        in_specs=[pl.BlockSpec(memory_space=pltpu.HBM) if fetch else entire]
        + [entire] * (shards - 1)
        + [pl.BlockSpec((rank, rows), lambda j: (0, 0))] * shards
        + [pl.BlockSpec((rank, block), lambda j: (0, j))],
        out_specs=(
            pl.BlockSpec((total, block), lambda j: (0, j)),
            pl.BlockSpec((1, block), lambda j: (0, j)),
        ),
        scratch_shapes=scratch,
        compiler_params=pltpu.CompilerParams(
            dimension_semantics=("arbitrary",), vmem_limit_bytes=34 * 1024 * 1024
        ),
        cost_estimate=pl.CostEstimate(
            flops=2 * total * columns * 256,
            bytes_accessed=4 * total * columns,
            transcendentals=0,
        ),
    )(*weights, *lows, high)


def norm_kernel(shards, *refs):
    zero, cols = shards
    pieces, out_ref, held = refs[:-2], refs[-2], refs[-1]
    rows = pieces[0].shape[0]
    for across in range(cols):
        column = lax.axis_index("cols") ^ across
        for along in range(zero):
            row = lax.rem(lax.axis_index("zero") - along + zero, zero)
            held[pl.ds((row * cols + column) * rows, rows), :] = pieces[across * zero + along][...]
    out_ref[...] = held[...].astype(out_ref.dtype)


def passed_round(array, axes, shards):
    return [array] + [
        lax.ppermute(array, axes, [(i, (i + shift) % shards) for i in range(shards)])
        for shift in range(1, shards)
    ]


def norm_of(pieces, shards):
    rows = pieces[0].shape[0] // 128
    out = pl.pallas_call(
        functools.partial(norm_kernel, shards),
        out_shape=jax.ShapeDtypeStruct((len(pieces) * rows, 128), jnp.bfloat16),
        scratch_shapes=[pltpu.VMEM((len(pieces) * rows, 128), jnp.float32)],
        compiler_params=pltpu.CompilerParams(vmem_limit_bytes=2 * 1024 * 1024),
        name="norm",
    )(*(piece.reshape(rows, 128) for piece in pieces))
    return out.reshape(-1)


def is_small(zero, cols, norm):
    return zero * cols <= 8 and cols & (cols - 1) == 0 and norm.shape[0] % 128 == 0


def per_device(
    zero, cols,
    weight_gate, low_gate, high_gate, weight_up, low_up, high_up, norm_train, norm_step,
):
    lows_gate = passed_round(low_gate.T, "zero", zero)
    lows_up = passed_round(low_up.T, "zero", zero)
    weights_gate = passed_round(weight_gate, "zero", zero)
    weights_up = passed_round(weight_up, "zero", zero)
    small = is_small(zero, cols, norm_train)
    if small:
        norm = added(norm_train, norm_step, weight_gate.size)
        line = [norm] + [
            lax.ppermute(norm, "cols", [(i, i ^ flip) for i in range(cols)])
            for flip in range(1, cols)
        ]
    else:
        norm = norm_train + norm_step
    serving_gate, column_gate = merge(weights_gate, lows_gate, high_gate, False)
    if small:
        line, column_gate = lax.optimization_barrier((line, column_gate))
        pieces = sum((passed_round(piece, "zero", zero) for piece in line), [])
    serving_up, column_up = merge(weights_up, lows_up, high_up, False)
    if small:
        serve_norm = norm_of(pieces, (zero, cols))
    else:
        serve_norm = lax.all_gather(
            norm.astype(jnp.bfloat16), ("zero", "cols"), axis=0, tiled=True
        )
    return (
        serving_gate,
        serving_up,
        column_gate.reshape(-1),
        column_up.reshape(-1),
        serve_norm,
    )


def solution(mesh):
    in_specs = (
        P(("job", "zero"), "cols"),
        P(("job", "zero"), None),
        P("job", "cols"),
        P(("job", "zero"), "cols"),
        P(("job", "zero"), None),
        P("job", "cols"),
        P(("job", "zero", "cols")),
        P(("job", "zero", "cols")),
    )
    out_specs = (
        P("job", "cols"),
        P("job", "cols"),
        P(("job", "cols")),
        P(("job", "cols")),
        P("job"),
    )
    body = functools.partial(per_device, mesh.shape["zero"], mesh.shape["cols"])
    return jax.shard_map(
        body, mesh=mesh, in_specs=in_specs, out_specs=out_specs, check_vma=False
    )
```
